32 devices in a mesh: batch: 4 (over y, x), seq: 4 (over z), head: 2 (over core).
Axes of the slice: x: 2, y: 2, z: 4, core: 2. Of those that a mesh axis runs over, the one named last changes fastest.
Arguments:
- queries: bfloat16 [1, 6144, 2048], P(None, ('batch', 'seq'), 'head'), parts along dimension 1, may hold values from -240 to 240
- keys: bfloat16 [1, 6144, 1024], P(None, ('batch', 'seq'), 'head'), parts along dimension 1, may hold values from -6 to 6
- values: bfloat16 [1, 6144, 1024], P(None, ('batch', 'seq'), 'head'), parts along dimension 1, may hold values from -6 to 6
- exit_layer: int32 [48], P(('batch', 'seq')), parts along dimension 0, may hold values from 0 to 1
- tile_order: int32 [48], P('batch'), parts along dimension 0, may hold values from 0 to 11, each once
Outputs:
- attended: bfloat16 [1, 6144, 2048], P(None, ('batch', 'seq'), 'head'), parts along dimension 1
- live_tiles: int32 [4], P('batch'), parts along dimension 0
The draws below stay inside these ranges and needn't reach their ends.
There are 4 independent parts, one for each index of `batch`. The reference program is written for one: setup_inputs(seed, part) draws one part's arguments, and reference() takes and returns one part's arrays. A program takes and returns all parts, laid end to end along the dimension named above; each array names one. Nothing has to cross between parts.
Inputs may be any that keep to these rules, and one draw needn't show every extreme that they name: Tile t covers tokens t * 128 to t * 128 + 127 of the token dimension; tile_order is a permutation of 0 to 11.
All inputs are finite; a program needn't handle non-finite values.
Results may differ from the reference program's by a relative error of at most 0.0049.
Values may be sent and summed in bfloat16 or wider, within the bound.
A program may use at most 128 MiB of HBM per device.

```python
import math
import jax
import jax.numpy as jnp
from jax import lax

LAYERS = 1
QH = 8
KVH = 4
HD = 256
TILE = 128
TOKENS = 1536
TILES = 12
KW = 1024


def draw_queries(key, part):
    query_key = jax.random.fold_in(key, 101)
    base = jnp.clip(jax.random.normal(query_key, (LAYERS, TOKENS, QH * HD), jnp.float32), -6.0, 6.0)
    return base.astype(jnp.bfloat16)


def draw_exit_layer(key, part):
    exit_key = jax.random.fold_in(key, 202)
    tile_ids = jnp.arange(TILES, dtype=jnp.int32)
    lowest = tile_ids * LAYERS // TILES
    spread = LAYERS + 1 - lowest
    raw_bits = jax.random.randint(exit_key, (TILES,), 0, 1 << 20, dtype=jnp.int32)
    return (lowest + raw_bits % spread).astype(jnp.int32)


def levels(own_key, shape, pieces, low, largest):
    def one(dim, parts):
        draws = jax.random.uniform(jax.random.fold_in(jax.random.fold_in(own_key, 6), dim), (parts,), jnp.float32, low / len(pieces), largest / len(pieces))
        return jnp.repeat(jnp.exp(draws), shape[dim] // parts).reshape((-1,) + (1,) * (len(shape) - dim - 1))

    gain = one(*pieces[0])
    for cut in pieces[1:]:
        gain = gain * one(*cut)
    return gain


def bell_draw(own_key, shape, width, reach, shards=(), held_as=jnp.bfloat16):
    drawn = width * jax.random.normal(own_key, shape, jnp.float32)
    if shards:
        drawn = drawn * levels(own_key, shape, shards, -0.22, 0.18)
    return jnp.clip(drawn, -reach, reach).astype(held_as)


def setup_inputs(seed: int = 0, part: int = 0) -> dict:
    streams_of = jax.random.split(jax.random.key(seed), 6)
    part_keys = jax.random.split(jax.random.fold_in(streams_of[5], part), 6)
    queries = draw_queries(jax.random.fold_in(jax.random.fold_in(streams_of[5], part), 71), part)
    keys = bell_draw(part_keys[1], (LAYERS, TOKENS, KW), 1.0, 6.0, ((1, 4), (2, 2)))
    values = bell_draw(part_keys[2], (LAYERS, TOKENS, KW), 1.0, 6.0, ((1, 4), (2, 2)))
    exit_layer = draw_exit_layer(jax.random.fold_in(jax.random.fold_in(streams_of[5], part), 71), part)
    tile_order = jax.random.permutation(part_keys[4], TILES).astype(jnp.int32)
    return dict(queries=queries, keys=keys, values=values, exit_layer=exit_layer, tile_order=tile_order)


softcap = 50.0
query_scale = 0.0625


def reference(queries, keys, values, exit_layer, tile_order):
    group_size = QH // KVH
    offsets = jnp.arange(TOKENS, dtype=jnp.int32)
    positions = (tile_order[offsets // TILE] * TILE + offsets % TILE).astype(jnp.int32)
    token_exits = exit_layer[offsets // TILE]
    block_rows = math.gcd(TOKENS, 512)
    outputs = []
    for layer_id in range(LAYERS):
        key_heads = keys[layer_id].reshape(TOKENS, KVH, HD).astype(jnp.float32)
        value_heads = values[layer_id].reshape(TOKENS, KVH, HD).astype(jnp.float32)
        query_blocks = queries[layer_id].reshape(TOKENS // block_rows, block_rows, KVH, group_size, HD)
        query_pos = positions.reshape(TOKENS // block_rows, block_rows)

        def one_block(operands):
            query_block, pos_block = operands
            scores = jnp.einsum("tkgd,skd->kgts", query_block.astype(jnp.float32), key_heads) * query_scale
            allowed = positions[None, :] <= pos_block[:, None]
            weights = jnp.where(allowed[None, None], jnp.exp(softcap * jnp.tanh(scores / softcap)), 0.0)
            denominator = jnp.sum(weights, axis=-1)
            rounded = lax.optimization_barrier(weights.astype(jnp.bfloat16))
            numerator = jnp.einsum("kgts,skd->kgtd", rounded.astype(jnp.float32), value_heads)
            output = numerator / denominator[..., None]
            return jnp.transpose(output, (2, 0, 1, 3)).reshape(block_rows, QH * HD)

        attended_layer = lax.map(one_block, (query_blocks, query_pos)).reshape(TOKENS, QH * HD)
        attended_layer = jnp.where((token_exits > layer_id)[:, None], attended_layer, 0.0)
        outputs.append(attended_layer.astype(jnp.bfloat16))
    live_tiles = jnp.stack([jnp.sum((exit_layer > layer_id).astype(jnp.int32)) for layer_id in range(LAYERS)])
    return jnp.stack(outputs), live_tiles.astype(jnp.int32)
```

```python
import functools
import math

import jax
import jax.numpy as jnp
from jax import lax
from jax.experimental import pallas as pl
from jax.experimental.pallas import tpu as pltpu
from jax.sharding import PartitionSpec as P

HD = 256
TILE = 128
SOFTCAP = 50.0
QUERY_SCALE = 0.0625
IN_SCALE = QUERY_SCALE / SOFTCAP
OUT_SCALE = SOFTCAP * math.log2(math.e)
MESH = pl.DeviceIdType.MESH


def kernel(
    n, order_ref, exit_ref, exits_vec, q_hbm, k_hbm, v_hbm, out_ref, live_ref,
    q_ref, kv, acc, den, exits, in_sem, send_sem, recv_sem, exit_send, exit_recv,
):
    me = lax.axis_index("seq")
    tiles = kv.shape[1]
    rows, q_width = q_ref.shape
    heads = q_width // HD
    group = heads // (k_hbm.shape[1] // HD)

    q_copy = pltpu.make_async_copy(q_hbm, q_ref, in_sem.at[2 * tiles])

    def own_copy(t, which):
        src = (k_hbm, v_hbm)[which]
        return pltpu.make_async_copy(
            src.at[pl.ds(t * TILE, TILE)], kv.at[me, t, which], in_sem.at[2 * t + which]
        )

    for t in range(tiles):
        for which in range(2):
            own_copy(t, which).start()
    q_copy.start()

    barrier = pltpu.get_barrier_semaphore()
    for d in range(1, n):
        pl.semaphore_signal(
            barrier, inc=1, device_id={"seq": lax.rem(me + d, n)}, device_id_type=MESH
        )
    pl.semaphore_wait(barrier, n - 1)

    def hop(owner, t, way):
        step = 1 if way == 0 else -1
        return pltpu.make_async_remote_copy(
            src_ref=kv.at[owner, t],
            dst_ref=kv.at[owner, t],
            send_sem=send_sem.at[way, owner, t],
            recv_sem=recv_sem.at[owner, t],
            device_id={"seq": jnp.clip(me + step, 0, n - 1)},
            device_id_type=MESH,
        )

    def can(way):
        return me < n - 1 if way == 0 else me > 0

    for t in range(tiles):
        for which in range(2):
            own_copy(t, which).wait()
        for way in range(2):
            @pl.when(can(way))
            def _():
                hop(me, t, way).start()

    def exit_copy(d):
        return pltpu.make_async_remote_copy(
            src_ref=exits_vec,
            dst_ref=exits.at[d - 1],
            send_sem=exit_send.at[d - 1],
            recv_sem=exit_recv.at[d - 1],
            device_id={"seq": lax.rem(me + d, n)},
            device_id_type=MESH,
        )

    for d in range(1, n):
        exit_copy(d).start()

    acc[...] = jnp.zeros_like(acc)
    den[...] = jnp.zeros_like(den)
    q_copy.wait()
    ahead = lax.broadcasted_iota(jnp.int32, (TILE, TILE), 1) - lax.broadcasted_iota(
        jnp.int32, (TILE, TILE), 0
    )

    def fold(owner, t):
        key_place = order_ref[owner * tiles + t]
        for i in range(rows // TILE):
            here = pl.ds(i * TILE, TILE)
            reach = (order_ref[me * tiles + i] - key_place) * TILE
            allowed = ahead <= reach
            for h in range(heads):
                cols = pl.ds(h * HD, HD)
                kv_cols = pl.ds((h // group) * HD, HD)
                scores = lax.dot_general(
                    q_ref[here, cols], kv[owner, t, 0, :, kv_cols],
                    (((1,), (1,)), ((), ())), preferred_element_type=jnp.float32,
                )
                weights = jnp.where(
                    allowed, jnp.exp2(OUT_SCALE * jnp.tanh(scores * IN_SCALE)), 0.0
                )
                den[h, here, :] += weights
                acc[here, cols] += jnp.dot(
                    weights.astype(jnp.bfloat16), kv[owner, t, 1, :, kv_cols],
                    preferred_element_type=jnp.float32,
                )

    @pl.loop(0, tiles)
    def _(t):
        fold(me, t)

    @pl.loop(1, n)
    def _(s):
        @pl.loop(0, tiles)
        def _(t):
            for way in range(2):
                owner = me - s if way == 0 else me + s

                @pl.when(owner >= 0 if way == 0 else owner < n)
                def _():
                    hop(owner, t, way).wait_recv()

                    @pl.when(can(way))
                    def _():
                        hop(owner, t, way).start()

            for way in range(2):
                owner = me - s if way == 0 else me + s

                @pl.when(owner >= 0 if way == 0 else owner < n)
                def _():
                    fold(owner, t)

    for i in range(rows // TILE):
        here = pl.ds(i * TILE, TILE)
        is_live = exit_ref[i] > 0
        for h in range(heads):
            cols = pl.ds(h * HD, HD)
            total = jnp.sum(den[h, here, :], axis=1, keepdims=True)
            result = acc[here, cols] / total
            out_ref[here, cols] = jnp.where(is_live, result, 0.0).astype(out_ref.dtype)

    count = jnp.sum((exits_vec[...] > 0).astype(jnp.int32))
    for d in range(1, n):
        exit_copy(d).wait()
        count += jnp.sum((exits[d - 1] > 0).astype(jnp.int32))
    live_ref[0] = count

    @pl.loop(0, n)
    def _(s):
        @pl.loop(0, tiles)
        def _(t):
            for way in range(2):
                owner = me - s if way == 0 else me + s

                @pl.when((owner >= 0 if way == 0 else owner < n) & can(way))
                def _():
                    hop(owner, t, way).wait_send()


def body(n, queries, keys, values, exit_layer, tile_order):
    rows, q_width = queries.shape[1:]
    kv_width = keys.shape[2]
    tiles = rows // TILE
    heads = q_width // HD
    exits_vec = jnp.pad(exit_layer, (0, TILE - tiles)).reshape(1, TILE)
    smem = pl.BlockSpec(memory_space=pltpu.SMEM)
    hbm = pl.BlockSpec(memory_space=pl.ANY)
    vmem = pl.BlockSpec(memory_space=pltpu.VMEM)
    attended, live = pl.pallas_call(
        functools.partial(kernel, n),
        out_shape=(
            jax.ShapeDtypeStruct((rows, q_width), jnp.bfloat16),
            jax.ShapeDtypeStruct((1,), jnp.int32),
        ),
        in_specs=[smem, smem, vmem, hbm, hbm, hbm],
        out_specs=(vmem, smem),
        scratch_shapes=[
            pltpu.VMEM((rows, q_width), jnp.bfloat16),
            pltpu.VMEM((n, tiles, 2, TILE, kv_width), jnp.bfloat16),
            pltpu.VMEM((rows, q_width), jnp.float32),
            pltpu.VMEM((heads, rows, TILE), jnp.float32),
            pltpu.VMEM((n - 1, 1, TILE), jnp.int32),
            pltpu.SemaphoreType.DMA((2 * tiles + 1,)),
            pltpu.SemaphoreType.DMA((2, n, tiles)),
            pltpu.SemaphoreType.DMA((n, tiles)),
            pltpu.SemaphoreType.DMA((n - 1,)),
            pltpu.SemaphoreType.DMA((n - 1,)),
        ],
        compiler_params=pltpu.CompilerParams(collective_id=0, has_side_effects=True),
        name="attend_line",
    )(tile_order, exit_layer, exits_vec, queries[0], keys[0], values[0])
    return attended[None], live


def solution(mesh):
    return jax.shard_map(
        functools.partial(body, mesh.shape["seq"]),
        mesh=mesh,
        in_specs=(
            P(None, ("batch", "seq"), "head"),
            P(None, ("batch", "seq"), "head"),
            P(None, ("batch", "seq"), "head"),
            P(("batch", "seq")),
            P("batch"),
        ),
        out_specs=(P(None, ("batch", "seq"), "head"), P("batch")),
        check_vma=False,
    )
```

```python
import functools
import math

import jax
import jax.numpy as jnp
from jax import lax
from jax.experimental import pallas as pl
from jax.experimental.pallas import tpu as pltpu
from jax.sharding import PartitionSpec as P

HD = 256
TILE = 128
SOFTCAP = 50.0
QUERY_SCALE = 0.0625
IN_SCALE = QUERY_SCALE / SOFTCAP
OUT_SCALE = SOFTCAP * math.log2(math.e)
MESH = pl.DeviceIdType.MESH


def kernel(
    n, order_ref, exits_vec, q_hbm, k_hbm, v_hbm, out_ref, live_ref,
    qb, kv, acc, den, done, exits, kv_sem, q_sem, send_sem, recv_sem,
    q_send, q_recv, o_send, o_recv, exit_send, exit_recv,
):
    me = lax.axis_index("seq")
    core = lax.axis_index("head")
    tiles = kv.shape[2]
    rows, q_half = qb.shape[1:]
    kv_half = kv.shape[5]
    heads = q_half // HD
    group = heads // (kv_half // HD)
    at_end = (me == 0) | (me == n - 1)
    serves = (me == 1) | (me == n - 2)
    end = jnp.where(me < n // 2, 0, n - 1)
    inward = jnp.where(me < n // 2, 1, -1)

    def peer(step):
        return {"seq": jnp.clip(me + step, 0, n - 1)}

    def own_copy(hh, t, which):
        src = (k_hbm, v_hbm)[which]
        return pltpu.make_async_copy(
            src.at[pl.ds(t * TILE, TILE), pl.ds(pl.multiple_of(hh * kv_half, kv_half), kv_half)],
            kv.at[me, hh, t, which],
            kv_sem.at[hh, t, which],
        )

    def own_queries(hh):
        return pltpu.make_async_copy(
            q_hbm.at[:, pl.ds(hh * q_half, q_half)], qb.at[hh], q_sem.at[hh]
        )

    first = core
    for hh in (first, 1 - first):
        for t in range(tiles):
            for which in range(2):
                own_copy(hh, t, which).start()
    for hh in range(2):
        own_queries(hh).start()

    barrier = pltpu.get_barrier_semaphore()
    for d in range(1, n):
        pl.semaphore_signal(
            barrier, inc=1, device_id={"seq": lax.rem(me + d, n)}, device_id_type=MESH
        )
    pl.semaphore_wait(barrier, n - 1)

    def hop(owner, hh, t, step):
        return pltpu.make_async_remote_copy(
            src_ref=kv.at[owner, hh, t],
            dst_ref=kv.at[owner, hh, t],
            send_sem=send_sem.at[(step + 1) // 2, owner, hh, t],
            recv_sem=recv_sem.at[owner, hh, t],
            device_id=peer(step),
            device_id_type=MESH,
        )

    def goes(hh, step):
        room = jnp.where(step > 0, n - 1 - me, me)
        return (room > 1) | ((room == 1) & (hh == 1))

    def send(owner, hh, t, step):
        @pl.when(goes(hh, step))
        def _():
            hop(owner, hh, t, step).start()

    def query_copy(t):
        part = pl.ds(t * TILE, TILE)
        return pltpu.make_async_remote_copy(
            src_ref=qb.at[0, part], dst_ref=qb.at[2, part],
            send_sem=q_send.at[t], recv_sem=q_recv.at[t],
            device_id=peer(inward), device_id_type=MESH,
        )

    def done_copy(t):
        part = pl.ds(t * TILE, TILE)
        return pltpu.make_async_remote_copy(
            src_ref=done.at[0, part], dst_ref=done.at[1, part],
            send_sem=o_send.at[t], recv_sem=o_recv.at[t],
            device_id=peer(-inward), device_id_type=MESH,
        )

    for t in range(tiles):
        for which in range(2):
            own_copy(first, t, which).wait()
        send(me, first, t, inward)
        send(me, first, t, -inward)
        if t == 0:
            own_queries(0).wait()

        @pl.when(at_end)
        def _():
            query_copy(t).start()

    def exit_copy(d):
        return pltpu.make_async_remote_copy(
            src_ref=exits_vec, dst_ref=exits.at[d - 1],
            send_sem=exit_send.at[d - 1], recv_sem=exit_recv.at[d - 1],
            device_id={"seq": lax.rem(me + d, n)}, device_id_type=MESH,
        )

    for t in range(tiles):
        for which in range(2):
            own_copy(1 - first, t, which).wait()
        send(me, 1 - first, t, -inward)

        @pl.when(at_end)
        def _():
            send(me, 1 - first, t, inward)

    for d in range(1, n):
        exit_copy(d).start()

    acc[...] = jnp.zeros_like(acc)
    den[...] = jnp.zeros_like(den)
    own_queries(1).wait()
    ahead = lax.broadcasted_iota(jnp.int32, (TILE, TILE), 1) - lax.broadcasted_iota(
        jnp.int32, (TILE, TILE), 0
    )

    def fold_into(slot, row_owner, owner, hh, t):
        key_place = order_ref[owner * tiles + t]
        for i in range(rows // TILE):
            here = pl.ds(i * TILE, TILE)
            reach = (order_ref[row_owner * tiles + i] - key_place) * TILE
            allowed = ahead <= reach
            for h in range(heads):
                cols = pl.ds(h * HD, HD)
                kv_cols = pl.ds((h // group) * HD, HD)
                scores = lax.dot_general(
                    qb[slot, here, cols], kv[owner, hh, t, 0, :, kv_cols],
                    (((1,), (1,)), ((), ())), preferred_element_type=jnp.float32,
                )
                weights = jnp.where(
                    allowed, jnp.exp2(OUT_SCALE * jnp.tanh(scores * IN_SCALE)), 0.0
                )
                den[slot, h, here, :] += weights
                acc[slot, here, cols] += jnp.dot(
                    weights.astype(jnp.bfloat16), kv[owner, hh, t, 1, :, kv_cols],
                    preferred_element_type=jnp.float32,
                )

    def fold(owner, hh, t, phase):
        low = jnp.where(at_end & (hh == 0), 1, 0)
        high = jnp.where(serves & (hh == 0) & (phase == 1), 2, 1)

        @pl.loop(low, high)
        def _(k):
            fold_into(
                jnp.where(k == 0, hh, 2), jnp.where(k == 0, me, end), owner, hh, t
            )

    def finish(slot, i, h):
        here = pl.ds(i * TILE, TILE)
        total = jnp.sum(den[slot, h, here, :], axis=1, keepdims=True)
        return (acc[slot, here, pl.ds(h * HD, HD)] / total).astype(jnp.bfloat16)

    def finish_served():
        for t in range(tiles):
            for h in range(heads):
                done[0, pl.ds(t * TILE, TILE), pl.ds(h * HD, HD)] = finish(2, t, h)
            if t > 0:
                done_copy(t - 1).start()

    def arrive(owner, hh, t, side, phase):
        @pl.when((owner >= 0) & (owner < n) & ~(at_end & (hh == 0)))
        def _():
            hop(owner, hh, t, side).wait_recv()
            send(owner, hh, t, -side)

    def take(owner, hh, t, phase):
        @pl.when((owner >= 0) & (owner < n) & ~(at_end & (hh == 0)))
        def _():
            fold(owner, hh, t, phase)

    near = []
    for s in (1, 2):
        for t in range(tiles):
            near.append((tiles * (s - 1) + t + 1.0, 1, s, t))
            if s == 1 or n > 4:
                near.append((tiles * 2 * (s - 1) + 2 * t + 1.1, -1, s, t))
    near.sort()

    @pl.loop(0, 2)
    def _(phase):
        hh = jnp.where(phase == 0, first, 1 - first)

        @pl.when(serves & (hh == 0) & (phase == 1))
        def _():
            for t in range(tiles):
                query_copy(t).wait_recv()

        @pl.loop(0, tiles)
        def _(t):
            fold(me, hh, t, phase)

        for _, sign, s, t in near:
            side = inward * sign
            owner = me + side * s
            arrive(owner, hh, t, side, phase)
            if sign == -1 and s == 1:
                @pl.when((phase == 0) & ~at_end)
                def _():
                    send(me, 1 - first, t, inward)
            take(owner, hh, t, phase)

        @pl.loop(3, n)
        def _(s):
            @pl.loop(0, tiles)
            def _(t):
                for sign in (1, -1) if n > 4 else (1,):
                    side = inward * sign
                    arrive(me + side * s, hh, t, side, phase)
                    take(me + side * s, hh, t, phase)

        @pl.when(serves & (hh == 0))
        def _():
            @pl.when(phase == 0)
            def _():
                for t in range(tiles):
                    query_copy(t).wait_recv()

                @pl.loop(0, n)
                def _(owner):
                    @pl.loop(0, tiles)
                    def _(t):
                        fold_into(2, end, owner, 0, t)

            finish_served()
            for h in range(heads):
                out_ref[pl.ds(0, TILE), pl.ds(h * HD, HD)] = finish(0, 0, h)
            done_copy(tiles - 1).start()

    for i in range(rows // TILE):
        for h in range(heads):
            out_ref[pl.ds(i * TILE, TILE), pl.ds(q_half + h * HD, HD)] = finish(1, i, h)

    @pl.when(~at_end)
    def _():
        for i in range(rows // TILE):
            for h in range(heads):
                out_ref[pl.ds(i * TILE, TILE), pl.ds(h * HD, HD)] = finish(0, i, h)

    count = jnp.sum((exits_vec[...] > 0).astype(jnp.int32))
    for d in range(1, n):
        exit_copy(d).wait()
        count += jnp.sum((exits[d - 1] > 0).astype(jnp.int32))
    live_ref[0] = count

    @pl.when(at_end)
    def _():
        for t in range(tiles):
            here = pl.ds(t * TILE, TILE)
            done_copy(t).wait_recv()
            out_ref[here, pl.ds(0, q_half)] = done[1, here, :]
            query_copy(t).wait_send()

    @pl.when(serves)
    def _():
        for t in range(tiles):
            done_copy(t).wait_send()

    for step in (1, -1):
        @pl.loop(0, n)
        def _(s):
            owner = me - step * s

            @pl.loop(0, 2)
            def _(hh):
                @pl.when((owner >= 0) & (owner < n) & goes(hh, step))
                def _():
                    @pl.loop(0, tiles)
                    def _(t):
                        hop(owner, hh, t, step).wait_send()


def body(n, queries, keys, values, exit_layer, tile_order):
    rows, q_width = queries.shape[1:]
    kv_half = keys.shape[2] // 2
    q_half = q_width // 2
    tiles = rows // TILE
    exits_vec = jnp.pad(exit_layer, (0, TILE - tiles)).reshape(1, TILE)
    smem = pl.BlockSpec(memory_space=pltpu.SMEM)
    hbm = pl.BlockSpec(memory_space=pl.ANY)
    vmem = pl.BlockSpec(memory_space=pltpu.VMEM)
    dma = pltpu.SemaphoreType.DMA
    attended, live = pl.pallas_call(
        functools.partial(kernel, n),
        out_shape=(
            jax.ShapeDtypeStruct((rows, q_width), jnp.bfloat16),
            jax.ShapeDtypeStruct((1,), jnp.int32),
        ),
        in_specs=[smem, vmem, hbm, hbm, hbm],
        out_specs=(vmem, smem),
        scratch_shapes=[
            pltpu.VMEM((3, rows, q_half), jnp.bfloat16),
            pltpu.VMEM((n, 2, tiles, 2, TILE, kv_half), jnp.bfloat16),
            pltpu.VMEM((3, rows, q_half), jnp.float32),
            pltpu.VMEM((3, q_half // HD, rows, TILE), jnp.float32),
            pltpu.VMEM((2, rows, q_half), jnp.bfloat16),
            pltpu.VMEM((n - 1, 1, TILE), jnp.int32),
            dma((2, tiles, 2)),
            dma((2,)),
            dma((2, n, 2, tiles)),
            dma((n, 2, tiles)),
            dma((tiles,)),
            dma((tiles,)),
            dma((tiles,)),
            dma((tiles,)),
            dma((n - 1,)),
            dma((n - 1,)),
        ],
        compiler_params=pltpu.CompilerParams(collective_id=0, has_side_effects=True),
        name="attend_line",
    )(tile_order, exits_vec, queries[0], keys[0], values[0])
    live_rows = jnp.repeat(exit_layer > 0, TILE, total_repeat_length=rows)
    attended = jnp.where(live_rows[:, None], attended, jnp.zeros((), jnp.bfloat16))
    return attended[None], live


def solution(mesh):
    return jax.shard_map(
        functools.partial(body, mesh.shape["seq"]),
        mesh=mesh,
        in_specs=(
            P(None, ("batch", "seq"), "head"),
            P(None, ("batch", "seq"), "head"),
            P(None, ("batch", "seq"), "head"),
            P(("batch", "seq")),
            P("batch"),
        ),
        out_specs=(P(None, ("batch", "seq"), "head"), P("batch")),
        check_vma=False,
    )
```

```python
import functools
import math

import jax
import jax.numpy as jnp
from jax import lax
from jax.experimental import pallas as pl
from jax.experimental.pallas import tpu as pltpu
from jax.sharding import PartitionSpec as P

HD = 256
TILE = 128
SOFTCAP = 50.0
QUERY_SCALE = 0.0625
IN_SCALE = QUERY_SCALE / SOFTCAP
OUT_SCALE = SOFTCAP * math.log2(math.e)
MESH = pl.DeviceIdType.MESH


def kernel(
    n, order_ref, exit_ref, exits_vec, q_hbm, k_hbm, v_hbm, out_ref, live_ref,
    qb, kv, acc, den, done, exits, kv_sem, q_sem, send_sem, recv_sem,
    q_send, q_recv, o_send, o_recv, exit_send, exit_recv,
):
    me = lax.axis_index("seq")
    core = lax.axis_index("head")
    tiles = kv.shape[2]
    heads, rows = qb.shape[1:3]
    q_half = heads * HD
    kv_half = kv.shape[5]
    at_end = (me == 0) | (me == n - 1)
    serves = (me == 1) | (me == n - 2)
    end = jnp.where(me < n // 2, 0, n - 1)
    inward = jnp.where(me < n // 2, 1, -1)

    def peer(step):
        return {"seq": jnp.clip(me + step, 0, n - 1)}

    def own_copy(hh, t, which):
        src = (k_hbm, v_hbm)[which]
        return pltpu.make_async_copy(
            src.at[pl.ds(t * TILE, TILE), pl.ds(pl.multiple_of(hh * kv_half, kv_half), kv_half)],
            kv.at[me, hh, t, which],
            kv_sem.at[hh, t, which],
        )

    def own_queries(hh, h):
        return pltpu.make_async_copy(
            q_hbm.at[:, pl.ds(hh * q_half + h * HD, HD)], qb.at[hh, h], q_sem.at[hh, h]
        )

    first = core
    for h in range(heads):
        own_queries(0, h).start()
    for hh in (first, 1 - first):
        for t in range(tiles):
            for which in range(2):
                own_copy(hh, t, which).start()
    for h in range(heads):
        own_queries(1, h).start()

    barrier = pltpu.get_barrier_semaphore()
    for d in range(1, n):
        pl.semaphore_signal(
            barrier, inc=1, device_id={"seq": lax.rem(me + d, n)}, device_id_type=MESH
        )
    pl.semaphore_wait(barrier, n - 1)

    def hop(owner, hh, t, step):
        return pltpu.make_async_remote_copy(
            src_ref=kv.at[owner, hh, t],
            dst_ref=kv.at[owner, hh, t],
            send_sem=send_sem.at[(step + 1) // 2, owner, hh, t],
            recv_sem=recv_sem.at[owner, hh, t],
            device_id=peer(step),
            device_id_type=MESH,
        )

    def goes(hh, step):
        room = jnp.where(step > 0, n - 1 - me, me)
        return (room > 1) | ((room == 1) & (hh == 1))

    def send(owner, hh, t, step):
        @pl.when(goes(hh, step))
        def _():
            hop(owner, hh, t, step).start()

    def query_copy(t):
        part = pl.ds(t * TILE, TILE)
        return pltpu.make_async_remote_copy(
            src_ref=qb.at[0, :, part], dst_ref=qb.at[2, :, part],
            send_sem=q_send.at[t], recv_sem=q_recv.at[t],
            device_id=peer(inward), device_id_type=MESH,
        )

    def done_copy(t):
        part = pl.ds(t * TILE, TILE)
        return pltpu.make_async_remote_copy(
            src_ref=done.at[0, part], dst_ref=done.at[1, part],
            send_sem=o_send.at[t], recv_sem=o_recv.at[t],
            device_id=peer(-inward), device_id_type=MESH,
        )

    for h in range(heads):
        own_queries(0, h).wait()

    for t in range(tiles):
        for which in range(2):
            own_copy(first, t, which).wait()
        send(me, first, t, inward)
        send(me, first, t, -inward)

    @pl.when(at_end)
    def _():
        for t in range(tiles):
            query_copy(t).start()

    def exit_copy(d):
        return pltpu.make_async_remote_copy(
            src_ref=exits_vec, dst_ref=exits.at[d - 1],
            send_sem=exit_send.at[d - 1], recv_sem=exit_recv.at[d - 1],
            device_id={"seq": lax.rem(me + d, n)}, device_id_type=MESH,
        )

    for t in range(tiles):
        for which in range(2):
            own_copy(1 - first, t, which).wait()
        send(me, 1 - first, t, -inward)

        @pl.when(at_end)
        def _():
            send(me, 1 - first, t, inward)

    for d in range(1, n):
        exit_copy(d).start()

    acc[...] = jnp.zeros_like(acc)
    den[...] = jnp.zeros_like(den)
    for h in range(heads):
        own_queries(1, h).wait()
    ahead = lax.broadcasted_iota(jnp.int32, (TILE, TILE), 1) - lax.broadcasted_iota(
        jnp.int32, (TILE, TILE), 0
    )

    def fold_into(slot, row_owner, owner, hh, t):
        key_place = order_ref[owner * tiles + t]
        over = jnp.stack(
            [
                ahead - (order_ref[row_owner * tiles + i] - key_place) * TILE
                for i in range(tiles)
            ]
        )
        stacked = (heads * rows, HD)
        scores = lax.dot_general(
            qb[slot].reshape(stacked), kv[owner, hh, t, 0],
            (((1,), (1,)), ((), ())), preferred_element_type=jnp.float32,
        ).reshape(heads, tiles, TILE, TILE)
        weights = jnp.where(
            over[None] <= 0, jnp.exp2(OUT_SCALE * jnp.tanh(scores * IN_SCALE)), 0.0
        ).reshape(heads * rows, TILE)
        den[slot] += weights
        acc[slot] += jnp.dot(
            weights.astype(jnp.bfloat16), kv[owner, hh, t, 1],
            preferred_element_type=jnp.float32,
        )

    def fold(owner, hh, t, phase):
        low = jnp.where(at_end & (hh == 0), 1, 0)
        high = jnp.where(serves & (hh == 0) & (phase == 1), 2, 1)

        @pl.loop(low, high)
        def _(k):
            fold_into(
                jnp.where(k == 0, hh, 2), jnp.where(k == 0, me, end), owner, hh, t
            )

    def finish(slot, i, h):
        here = pl.ds(h * rows + i * TILE, TILE)
        total = jnp.sum(den[slot, here, :], axis=1, keepdims=True)
        return (acc[slot, here, :] / total).astype(jnp.bfloat16)

    def keep(slot, i, h):
        out_ref[pl.ds(i * TILE, TILE), pl.ds(slot * q_half + h * HD, HD)] = live_only(
            i, finish(slot, i, h)
        )

    def live_only(i, rows_out):
        return jnp.where(exit_ref[i] > 0, rows_out, jnp.zeros_like(rows_out))

    def late_fold(part, parts):
        share = n * tiles // parts

        @pl.loop(part * share, (part + 1) * share)
        def _(k):
            fold_into(2, end, k // tiles, 0, k % tiles)

    def finish_served():
        for t in range(tiles):
            for h in range(heads):
                done[0, pl.ds(t * TILE, TILE), pl.ds(h * HD, HD)] = finish(2, t, h)
            if t > 0:
                done_copy(t - 1).start()
        for h in range(heads):
            keep(0, 0, h)
        done_copy(tiles - 1).start()

    def arrive(owner, hh, t, side, phase):
        @pl.when((owner >= 0) & (owner < n) & ~(at_end & (hh == 0)))
        def _():
            hop(owner, hh, t, side).wait_recv()
            send(owner, hh, t, -side)

    def take(owner, hh, t, phase):
        @pl.when((owner >= 0) & (owner < n) & ~(at_end & (hh == 0)))
        def _():
            fold(owner, hh, t, phase)

    near = []
    for s in (1, 2):
        for t in range(tiles):
            near.append((tiles * (s - 1) + t + 1.0, 1, s, t))
            if s == 1 or n > 4:
                near.append((tiles * 2 * (s - 1) + 2 * t + 1.1, -1, s, t))
    near.sort()

    @pl.loop(0, 2)
    def _(phase):
        hh = jnp.where(phase == 0, first, 1 - first)

        @pl.when(serves & (phase == 1))
        def _():
            for t in range(tiles):
                query_copy(t).wait_recv()

        @pl.loop(0, tiles)
        def _(t):
            fold(me, hh, t, phase)

            @pl.when(serves & (phase == 1) & (core == 0))
            def _():
                late_fold(t, 2 * tiles)

        for _, sign, s, t in near:
            side = inward * sign
            owner = me + side * s
            arrive(owner, hh, t, side, phase)
            if sign == -1 and s == 1:
                if t == tiles - 1:
                    @pl.when((phase == 0) & ~at_end)
                    def _():
                        for own_t in range(tiles):
                            send(me, 1 - first, own_t, inward)
            take(owner, hh, t, phase)
            if sign == 1 and s == 1:
                @pl.when(serves & (phase == 1) & (core == 0))
                def _():
                    late_fold(tiles + t, 2 * tiles)

                    if t == tiles - 1:
                        finish_served()

        @pl.loop(3, n)
        def _(s):
            @pl.loop(0, tiles)
            def _(t):
                for sign in (1, -1) if n > 4 else (1,):
                    side = inward * sign
                    arrive(me + side * s, hh, t, side, phase)
                    take(me + side * s, hh, t, phase)

        @pl.when(serves & (hh == 0) & (phase == 1))
        def _():
            finish_served()

    for i in range(rows // TILE):
        for h in range(heads):
            keep(1, i, h)

    @pl.when(~at_end)
    def _():
        for i in range(rows // TILE):
            for h in range(heads):
                keep(0, i, h)

    count = jnp.sum((exits_vec[...] > 0).astype(jnp.int32))
    for d in range(1, n):
        exit_copy(d).wait()
        count += jnp.sum((exits[d - 1] > 0).astype(jnp.int32))
    live_ref[0] = count

    @pl.when(at_end)
    def _():
        for t in range(tiles):
            here = pl.ds(t * TILE, TILE)
            done_copy(t).wait_recv()
            out_ref[here, pl.ds(0, q_half)] = live_only(t, done[1, here, :])
            query_copy(t).wait_send()

    @pl.when(serves)
    def _():
        for t in range(tiles):
            done_copy(t).wait_send()

    for step in (1, -1):
        @pl.loop(0, n)
        def _(s):
            owner = me - step * s

            @pl.loop(0, 2)
            def _(hh):
                @pl.when((owner >= 0) & (owner < n) & goes(hh, step))
                def _():
                    @pl.loop(0, tiles)
                    def _(t):
                        hop(owner, hh, t, step).wait_send()


def body(n, queries, keys, values, exit_layer, tile_order):
    rows, q_width = queries.shape[1:]
    kv_half = keys.shape[2] // 2
    q_half = q_width // 2
    tiles = rows // TILE
    exits_vec = jnp.pad(exit_layer, (0, TILE - tiles)).reshape(1, TILE)
    smem = pl.BlockSpec(memory_space=pltpu.SMEM)
    hbm = pl.BlockSpec(memory_space=pl.ANY)
    vmem = pl.BlockSpec(memory_space=pltpu.VMEM)
    dma = pltpu.SemaphoreType.DMA
    attended, live = pl.pallas_call(
        functools.partial(kernel, n),
        out_shape=(
            jax.ShapeDtypeStruct((rows, q_width), jnp.bfloat16),
            jax.ShapeDtypeStruct((1,), jnp.int32),
        ),
        in_specs=[smem, smem, vmem, hbm, hbm, hbm],
        out_specs=(vmem, smem),
        scratch_shapes=[
            pltpu.VMEM((3, q_half // HD, rows, HD), jnp.bfloat16),
            pltpu.VMEM((n, 2, tiles, 2, TILE, kv_half), jnp.bfloat16),
            pltpu.VMEM((3, rows * q_half // HD, HD), jnp.float32),
            pltpu.VMEM((3, rows * q_half // HD, TILE), jnp.float32),
            pltpu.VMEM((2, rows, q_half), jnp.bfloat16),
            pltpu.VMEM((n - 1, 1, TILE), jnp.int32),
            dma((2, tiles, 2)),
            dma((2, q_half // HD)),
            dma((2, n, 2, tiles)),
            dma((n, 2, tiles)),
            dma((tiles,)),
            dma((tiles,)),
            dma((tiles,)),
            dma((tiles,)),
            dma((n - 1,)),
            dma((n - 1,)),
        ],
        compiler_params=pltpu.CompilerParams(
            collective_id=0, has_side_effects=True, vmem_limit_bytes=64_000_000
        ),
        name="attend_line",
    )(tile_order, exit_layer, exits_vec, queries[0], keys[0], values[0])
    return attended[None], live


def solution(mesh):
    return jax.shard_map(
        functools.partial(body, mesh.shape["seq"]),
        mesh=mesh,
        in_specs=(
            P(None, ("batch", "seq"), "head"),
            P(None, ("batch", "seq"), "head"),
            P(None, ("batch", "seq"), "head"),
            P(("batch", "seq")),
            P("batch"),
        ),
        out_specs=(P(None, ("batch", "seq"), "head"), P("batch")),
        check_vma=False,
    )
```
